32 devices in a mesh: patch: 16 (over z, y, x), width: 2 (over core).
Axes of the slice: x: 2, y: 2, z: 4, core: 2. Of those that a mesh axis runs over, the one named last changes fastest.
Arguments:
- node_latents: bfloat16 [512, 2048], P('width', 'patch'), may hold values from -6 to 6
- edge_latents: bfloat16 [512, 16384], P('width', 'patch'), may hold values from -6 to 6
- senders: int32 [16384], P('patch'), may hold values from 0 to 2047, as said below
- receivers: int32 [16384], P('patch'), may hold values from 0 to 2047, as said below
- edge_count: int32 [16], P('patch'), may hold values from 512 to 1024, as said below
- edge_in_weight: bfloat16 [2, 512, 1536], P(None, 'width'), may hold values from -0.15625 to 0.15625
- edge_in_bias: float32 [2, 512], P(None, 'width'), may hold values from -3 to 3
- edge_out_weight: bfloat16 [2, 512, 512], P(None, 'width'), may hold values from -0.25 to 0.25
- edge_out_bias: float32 [2, 512], P(None, 'width'), may hold values from -3 to 3
- edge_gain: float32 [2, 512], P(None, 'width'), may hold values from 0.1 to 1.9
- edge_shift: float32 [2, 512], P(None, 'width'), may hold values from -3 to 3
- node_in_weight: bfloat16 [2, 512, 1024], P(None, 'width'), may hold values from -0.1875 to 0.1875
- node_in_bias: float32 [2, 512], P(None, 'width'), may hold values from -3 to 3
- node_out_weight: bfloat16 [2, 512, 512], P(None, 'width'), may hold values from -0.25 to 0.25
- node_out_bias: float32 [2, 512], P(None, 'width'), may hold values from -3 to 3
- node_gain: float32 [2, 512], P(None, 'width'), may hold values from 0.1 to 1.9
- node_shift: float32 [2, 512], P(None, 'width'), may hold values from -3 to 3
Outputs:
- nodes_out: bfloat16 [512, 2048], P('width', 'patch')
- edges_out: bfloat16 [512, 16384], P('width', 'patch')
The draws below stay inside these ranges and needn't reach their ends.
Inputs may be any that keep to these rules, and one draw needn't show every extreme that they name: `senders`: the sender of a slot of patch p is a node of patch p, of patch p - 1 or p + 1 (counted around, modulo the number of patches), or one of the first 16 nodes of some patch. `receivers`: row r names a node of patch r // 1024, from (r // 1024) * 128 to that plus 128 - 1. Slots p * 1024 to p * 1024 + edge_count[p] - 1 of patch p are live, the rest are padding; some patch has all 1024 slots live.
All inputs are finite; a program needn't handle non-finite values.
Results may differ from the reference program's by a relative error of at most 0.014.
Values may be sent and summed in bfloat16 or wider, within the bound.
A program may use at most 64 MiB of HBM per device.

```python
import jax
import jax.numpy as jnp
from jax import lax

D = 512
H = 512
LAYERS = 2
NODE_DEV = 128
COARSE = 16
EDGE_DEV = 1024
NODES = 2048
EDGES = 16384


def draw_graph(key):
    base = jax.random.fold_in(key, 17)
    keys = jax.random.split(base, 8)
    patches = NODES // NODE_DEV
    slots = jnp.arange(EDGES, dtype=jnp.int32)
    block = slots // EDGE_DEV
    local = jax.random.randint(keys[0], (EDGES,), 0, NODE_DEV).astype(jnp.int32)
    receivers = block * NODE_DEV + local
    kinds = jax.random.randint(keys[1], (EDGES,), 0, 4)
    offset = jax.random.randint(keys[2], (EDGES,), -8, 9).astype(jnp.int32)
    near = block * NODE_DEV + (local + offset) % NODE_DEV
    sideways = jax.random.randint(keys[3], (EDGES,), 0, 2).astype(jnp.int32) * 2 - 1
    beside = (block + sideways) % patches * NODE_DEV + jax.random.randint(keys[4], (EDGES,), 0, NODE_DEV).astype(jnp.int32)
    random_patch = jax.random.randint(keys[5], (EDGES,), 0, patches).astype(jnp.int32)
    opposite = ((block + patches // 2) % patches).astype(jnp.int32)
    toward = jax.random.randint(keys[7], (EDGES,), 0, 2)
    far_patch = jnp.where(toward == 1, opposite, random_patch)
    anywhere = far_patch * NODE_DEV + jax.random.randint(keys[6], (EDGES,), 0, COARSE).astype(jnp.int32)
    senders = jnp.where(kinds < 2, near, jnp.where(kinds == 2, beside, anywhere))
    return (senders.astype(jnp.int32), receivers.astype(jnp.int32))


def draw_senders(key, part):
    return draw_graph(key)[0]


def draw_receivers(key, part):
    return draw_graph(key)[1]


def draw_edge_count(key, part):
    patches = NODES // NODE_DEV
    first, second = jax.random.split(jax.random.fold_in(key, 29))
    counts = jax.random.randint(first, (patches,), EDGE_DEV // 2, EDGE_DEV + 1).astype(jnp.int32)
    filled = jax.random.randint(second, (), 0, patches)
    return jnp.where(jnp.arange(patches) == filled, EDGE_DEV, counts).astype(jnp.int32)


def levels(rng, extent, shards, low, largest):
    def one(dim, shards_of):
        draws = jax.random.uniform(jax.random.fold_in(jax.random.fold_in(rng, 6), dim), (shards_of,), jnp.float32, low / len(shards), largest / len(shards))
        return jnp.repeat(jnp.exp(draws), extent[dim] // shards_of).reshape((-1,) + (1,) * (len(extent) - dim - 1))

    level = one(*shards[0])
    for cut in shards[1:]:
        level = level * one(*cut)
    return level


def gaussian(rng, shape, width, bound, shards=(), held_as=jnp.bfloat16):
    drawn = width * jax.random.normal(rng, shape, jnp.float32)
    if shards:
        drawn = drawn * levels(rng, shape, shards, -0.22, 0.18)
    return jnp.clip(drawn, -bound, bound).astype(held_as)


def setup_inputs(seed: int = 0) -> dict:
    key_of = jax.random.split(jax.random.key(seed), 18)
    return {
        "node_latents": gaussian(key_of[0], (D, NODES), 1.0, 6.0, ((0, 2), (1, 16))),
        "edge_latents": gaussian(key_of[1], (D, EDGES), 1.0, 6.0, ((0, 2), (1, 16))),
        "senders": draw_senders(jax.random.fold_in(key_of[17], 71), 0),
        "receivers": draw_receivers(jax.random.fold_in(key_of[17], 71), 0),
        "edge_count": draw_edge_count(jax.random.fold_in(key_of[17], 71), 0),
        "edge_in_weight": gaussian(key_of[5], (LAYERS, H, 3 * D), (3 * D) ** -0.5, 0.15625, ((1, 2),)),
        "edge_in_bias": gaussian(key_of[6], (LAYERS, H), 0.5, 3.0, ((1, 2),), jnp.float32),
        "edge_out_weight": gaussian(key_of[7], (LAYERS, H, D), H ** -0.5, 0.25, ((1, 2),)),
        "edge_out_bias": gaussian(key_of[8], (LAYERS, D), 0.5, 3.0, ((1, 2),), jnp.float32),
        "edge_gain": jnp.clip(1.0 + 0.18 * jax.random.normal(key_of[9], (LAYERS, D), jnp.float32), 0.1, 1.9),
        "edge_shift": gaussian(key_of[10], (LAYERS, D), 0.5, 3.0, ((1, 2),), jnp.float32),
        "node_in_weight": gaussian(key_of[11], (LAYERS, H, 2 * D), (2 * D) ** -0.5, 0.1875, ((1, 2),)),
        "node_in_bias": gaussian(key_of[12], (LAYERS, H), 0.5, 3.0, ((1, 2),), jnp.float32),
        "node_out_weight": gaussian(key_of[13], (LAYERS, H, D), H ** -0.5, 0.25, ((1, 2),)),
        "node_out_bias": gaussian(key_of[14], (LAYERS, D), 0.5, 3.0, ((1, 2),), jnp.float32),
        "node_gain": jnp.clip(1.0 + 0.18 * jax.random.normal(key_of[15], (LAYERS, D), jnp.float32), 0.1, 1.9),
        "node_shift": gaussian(key_of[16], (LAYERS, D), 0.5, 3.0, ((1, 2),), jnp.float32),
    }


def layer_norm(values, gain, shift):
    mean = lax.optimization_barrier(jnp.sum(values, axis=-1, keepdims=True)) / D
    square = lax.optimization_barrier(jnp.sum(values * values, axis=-1, keepdims=True)) / D
    return (values - mean) * jax.lax.rsqrt(square - mean * mean + 1e-05) * gain + shift

def reference(node_latents, edge_latents, senders, receivers, edge_count, edge_in_weight, edge_in_bias, edge_out_weight, edge_out_bias, edge_gain, edge_shift, node_in_weight, node_in_bias, node_out_weight, node_out_bias, node_gain, node_shift):
    slots = jnp.arange(EDGES, dtype=jnp.int32)
    live = slots % EDGE_DEV < edge_count[slots // EDGE_DEV]
    nodes = node_latents.T
    edges = edge_latents.T
    for layer in range(LAYERS):
        w_edge = edge_in_weight[layer].T
        w_node = node_in_weight[layer].T
        sender_part = jnp.dot(nodes, w_edge[D:2 * D], preferred_element_type=jnp.float32).astype(jnp.bfloat16)
        receiver_part = jnp.dot(nodes, w_edge[2 * D:], preferred_element_type=jnp.float32).astype(jnp.bfloat16)
        node_first = jnp.dot(nodes, w_node[:D], preferred_element_type=jnp.float32)
        before = jnp.dot(edges, w_edge[:D], preferred_element_type=jnp.float32)
        before = before + sender_part[senders].astype(jnp.float32) + receiver_part[receivers].astype(jnp.float32) + edge_in_bias[layer]
        edge_hidden = jax.nn.silu(before).astype(jnp.bfloat16)
        edge_mlp = jnp.dot(edge_hidden, edge_out_weight[layer], preferred_element_type=jnp.float32) + edge_out_bias[layer]
        updated = edges.astype(jnp.float32) + layer_norm(edge_mlp, edge_gain[layer], edge_shift[layer])
        edges = jnp.where(live[:, None], updated, jnp.float32(0.0)).astype(jnp.bfloat16)
        aggregate = jax.ops.segment_sum(edges.astype(jnp.float32), receivers, num_segments=NODES).astype(jnp.bfloat16)
        node_before = node_first + jnp.dot(aggregate, w_node[D:], preferred_element_type=jnp.float32) + node_in_bias[layer]
        node_hidden = jax.nn.silu(node_before).astype(jnp.bfloat16)
        node_mlp = jnp.dot(node_hidden, node_out_weight[layer], preferred_element_type=jnp.float32) + node_out_bias[layer]
        nodes = (nodes.astype(jnp.float32) + layer_norm(node_mlp, node_gain[layer], node_shift[layer])).astype(jnp.bfloat16)
    return (nodes.T, edges.T)
```

```python
import functools

import jax
import jax.numpy as jnp
from jax import lax
from jax.experimental import pallas as pl
from jax.experimental.pallas import tpu as pltpu
from jax.sharding import PartitionSpec as P

MESH = pl.DeviceIdType.MESH
epsilon = 1e-05
bf16 = jnp.bfloat16
f32 = jnp.float32


def dot(left, right, dims=((1,), (0,))):
    return lax.dot_general(left, right, (dims, ((), ())), preferred_element_type=f32)


def silu(v):
    h = 0.5 * v
    return h + h * jnp.tanh(h)


def layer_norm(values, gain, shift):
    width = values.shape[0]
    mean = jnp.sum(values, axis=0, keepdims=True) / width
    square = jnp.sum(values * values, axis=0, keepdims=True) / width
    return (values - mean) * lax.rsqrt(square - mean * mean + epsilon) * gain + shift


def kernel(
    patches,
    nodes_in,
    edges_in,
    senders_in,
    receivers_in,
    count_in,
    wi_in,
    wo_in,
    vi_in,
    vo_in,
    *rest,
):
    vector_in = rest[:8]
    nodes_out, edges_out = rest[8:10]
    (
        nodes,
        edges,
        weights,
        vectors,
        columns,
        halo,
        coarse,
        part_send,
        coarse_send,
        agg_send,
        agg_recv,
        partial,
        own,
        hot_own,
        hot_far,
        incidence,
        before,
        graph_ref,
        count_ref,
        wo_turned,
        vo_turned,
        graph_sem,
        local_sem,
        w_send,
        w_recv,
        halo_send,
        halo_recv,
        coarse_send_sem,
        coarse_recv_sem,
        relay_send,
        relay_recv,
        agg_sems,
        out_sems,
        mate,
        all_in,
    ) = rest[10:]
    layers = weights.shape[0]
    half = nodes_in.shape[0]
    width = 2 * half
    rows = nodes_in.shape[1]
    slots = edges_in.shape[1]
    mine = slots // 2
    top = coarse_send.shape[1]
    far = patches - 3
    lead = 1

    me = lax.axis_index("patch")
    odd = lax.rem(me, 2)
    core = lax.axis_index("width")
    other = 1 - core
    here = pl.ds(pl.multiple_of(core * half, half), half)
    there = pl.ds(pl.multiple_of(other * half, half), half)
    my_slots = pl.ds(pl.multiple_of(core * mine, mine), mine)
    other_slots = pl.ds(pl.multiple_of(other * mine, mine), mine)

    def remote(src, dst, send, recv, patch, width_index):
        return pltpu.make_async_remote_copy(
            src_ref=src,
            dst_ref=dst,
            send_sem=send,
            recv_sem=recv,
            device_id={"patch": patch, "width": width_index},
            device_id_type=MESH,
        )

    at_sender, at_edge, at_receiver, at_wo, at_node, at_aggregate, at_vo = (
        slice(k * width, (k + 1) * width) for k in range(7)
    )

    def weight(source, layer, first_column, target, count=1):
        from_ = source.at[layer, :, pl.ds(first_column, count * width)]
        to = weights.at[layer, here, pl.ds(target.start, count * width)]
        return from_, to

    def layer_rest(layer):
        return [
            weight(wo_in, layer, 0, at_wo),
            weight(vi_in, layer, 0, at_node, 2),
            weight(vo_in, layer, 0, at_vo),
        ]

    def layer_ends(layer):
        return [
            weight(wi_in, layer, 0, at_edge),
            weight(wi_in, layer, 2 * width, at_receiver),
        ]

    groups = [
        ("nodes", [(nodes_in, nodes.at[here])], nodes.at[there]),
        ("sender", [weight(wi_in, 0, width, at_sender)], weights.at[0, there, at_sender]),
        ("ends", layer_ends(0), weights.at[0, there, pl.ds(width, 2 * width)]),
        ("edges", None, edges.at[there]),
        (
            "vectors",
            [(source, vectors.at[index, :, here]) for index, source in enumerate(vector_in)],
            vectors.at[:, :, there],
        ),
        ("rest", layer_rest(0), weights.at[0, there, pl.ds(3 * width, 4 * width)]),
    ]
    for layer in range(1, layers):
        groups.append(
            (
                layer,
                [weight(wi_in, layer, width, at_sender)] + layer_ends(layer) + layer_rest(layer),
                weights.at[layer, there],
            )
        )
    place = {group[0]: index for index, group in enumerate(groups)}
    send_of = {"nodes": 0, "edges": 1, "vectors": 2}
    mine_of = {
        "nodes": nodes.at[here],
        "sender": weights.at[0, here, at_sender],
        "ends": weights.at[0, here, pl.ds(width, 2 * width)],
        "edges": edges.at[here],
        "vectors": vectors.at[:, :, here],
        "rest": weights.at[0, here, pl.ds(3 * width, 4 * width)],
    } | {layer: weights.at[layer, here] for layer in range(1, layers)}

    barrier = pltpu.get_barrier_semaphore()

    @pl.when(core == lead)
    def _():
        pl.semaphore_signal(barrier, inc=1, device_id={"patch": me, "width": other}, device_id_type=MESH)

    def greet(step, carry):
        target = lax.rem(me + step, patches)

        @pl.when((target != 0) | (me == 1))
        def _():
            pl.semaphore_signal(
                pltpu.get_barrier_semaphore(),
                inc=1,
                device_id={"patch": target, "width": lead},
                device_id_type=MESH,
            )

        return carry

    lax.fori_loop(1, patches, greet, 0)

    count_copy = pltpu.make_async_copy(count_in, count_ref, graph_sem.at[1])
    graph_copies = [
        pltpu.make_async_copy(source, graph_ref.at[pl.ds(k, 1)], graph_sem.at[0])
        for k, source in enumerate((senders_in, receivers_in))
    ]

    def locals_of(index):
        name, copies, _ = groups[index]
        if name == "edges":
            copies = [(edges_in.at[:, my_slots], edges.at[here])]
        return [pltpu.make_async_copy(source, target, local_sem.at[index]) for source, target in copies]

    for index in range(2):
        for copy in locals_of(index):
            copy.start()
    for copy in [count_copy] + graph_copies:
        copy.start()
    for index in range(2, len(groups)):
        for copy in locals_of(index):
            copy.start()

    @pl.when(core != lead)
    def _():
        pl.semaphore_wait(barrier, 1)
        pl.semaphore_signal(mate, inc=1, device_id={"patch": me, "width": lead}, device_id_type=MESH)

    @pl.when(core == lead)
    def _():
        pl.semaphore_wait(mate, 1)

    for index, (name, copies, _) in enumerate(groups):
        if name == "edges":
            copies = [(edges_in.at[:, other_slots], edges.at[here])]
        for source, target in copies:
            remote(source, target, w_send.at[send_of.get(name, 3)], w_recv.at[index], me, other).start()

    def local_arrive(name):
        ref = mine_of[name]
        pltpu.make_async_copy(ref, ref, local_sem.at[place[name]]).wait()

    def arrive(name):
        if name not in ("nodes", "sender"):
            local_arrive(name)
        ref = groups[place[name]][2]
        remote(ref, ref, w_send.at[send_of.get(name, 3)], w_recv.at[place[name]], me, other).wait_recv()

    def hot(index, iota):
        return jnp.where(iota == index, 1.0, 0.0).astype(bf16)

    def masks():
        count_copy.wait()
        pltpu.make_async_copy(graph_ref, graph_ref, graph_sem.at[0]).wait()
        sender = graph_ref[0:1, my_slots]
        receiver = graph_ref[1:2, my_slots] - me * rows
        slot = lax.broadcasted_iota(jnp.int32, (1, mine), 1) + core * mine
        live = slot < count_ref[0]
        owner = sender // rows
        within = sender - owner * rows
        distance = lax.rem(me - owner + patches, patches)
        node_iota = lax.broadcasted_iota(jnp.int32, (rows, mine), 0)
        hot_own[:rows] = hot(jnp.where(distance == 0, within, -1), node_iota)
        hot_own[rows:] = hot(receiver, node_iota)
        hot_far[:rows] = hot(jnp.where(distance == 1, within, -1), node_iota)
        hot_far[rows : 2 * rows] = hot(jnp.where(distance == patches - 1, within, -1), node_iota)
        far_index = jnp.where((distance >= 2) & (distance <= patches - 2), (distance - 2) * top + within, -1)
        hot_far[2 * rows :] = hot(far_index, lax.broadcasted_iota(jnp.int32, (coarse.shape[1], mine), 0))
        incidence[...] = hot(jnp.where(live, receiver, -1), node_iota)
        return live

    pad = coarse.shape[1] - far * top
    if pad:
        for layer in range(layers):
            coarse[layer, far * top :, :] = jnp.zeros((pad, width), bf16)

    def halo_part(layer, side):
        return halo.at[layer, :, pl.ds(pl.multiple_of(side * rows, rows), rows)]

    def halo_copy(layer, side):
        return remote(
            part_send.at[layer],
            halo_part(layer, side),
            halo_send.at[layer],
            halo_recv.at[layer, side],
            lax.rem(me + 1 + side * (patches - 2), patches),
            lead,
        )

    def halo_arrival(layer, side):
        ref = halo_part(layer, side)
        return remote(ref, ref, halo_send.at[layer], halo_recv.at[layer, side], me, other)

    def coarse_part(layer):
        return coarse.at[layer, pl.ds(0, far * top)]

    def spread_coarse(layer):
        def send(target, step):
            remote(
                coarse_send.at[layer],
                coarse.at[layer, pl.ds(pl.multiple_of((step - 2) * top, top), top)],
                coarse_send_sem.at[layer],
                coarse_recv_sem.at[layer],
                target,
                1 - lead,
            ).start()

        def spread(turn, carry):
            step = patches - 2 - turn
            pl.when(me + step < patches)(lambda: send(me + step, step))
            pl.when(me - step >= 0)(lambda: send(me - step, patches - step))
            return carry

        lax.fori_loop(0, far, spread, 0)

    def send_halo(layer):
        if layer == 0:
            pl.semaphore_wait(barrier, jnp.where(me == 0, 2, 2 * (patches - 1)))

            @pl.when(me != 0)
            def _():
                pl.semaphore_signal(
                    all_in, inc=1, device_id={"patch": me, "width": other}, device_id_type=MESH
                )

            @pl.when(me == 1)
            def _():
                pl.semaphore_signal(all_in, inc=1, device_id={"patch": 0, "width": other}, device_id_type=MESH)
                halo_arrival(0, 0).wait_recv()
                remote(
                    halo_part(0, 0), halo_part(0, 1), halo_send.at[0], halo_recv.at[0, 1], patches - 1, lead
                ).start()

            pl.when(me != 0)(halo_copy(0, 1 - odd).start)
        else:
            halo_copy(layer, 1 - odd).start()
        halo_copy(layer, odd).start()

    def send_coarse(layer):
        if layer == 0:
            pl.semaphore_wait(all_in, 1)
        spread_coarse(layer)

    def column(index, layer):
        position = index * layers + layer
        return columns[:, position : position + 1]

    wide = [(k * mine // 2, (k + 1) * mine // 2) for k in range(2)]
    for layer in range(layers):
        if layer == 0:
            local_arrive("nodes")
            local_arrive("sender")
            arrive("nodes")
            arrive("sender")
        else:
            arrive(layer)
        part = dot(weights[layer, :, at_sender], nodes[...])
        part_send[layer] = part.astype(bf16)
        coarse_send[layer] = part.T[:top].astype(bf16)
        pl.when(core == lead)(functools.partial(send_halo, layer))
        pl.when(core != lead)(functools.partial(send_coarse, layer))
        if layer == 0:
            live = masks()
            arrive("ends")
        own[:, :rows] = part.astype(bf16)
        own[:, rows:] = dot(weights[layer, :, at_receiver], nodes[...]).astype(bf16)
        if layer == 0:
            arrive("edges")
            arrive("vectors")
            flat = vectors[...].reshape(8 * layers, width)
            columns[...] = flat.T
        before[...] = (
            dot(weights[layer, :, at_edge], edges[...]) + dot(own[...], hot_own[...]) + column(0, layer)
        )
        if layer == 0:
            arrive("rest")
        node_first = dot(weights[layer, :, at_node], nodes[...]) + column(4, layer)
        wo_turned[...] = weights[layer, :, at_wo].T
        vo_turned[...] = weights[layer, :, at_vo].T

        every = coarse_part(layer)
        all_coarse = remote(
            every, every, coarse_send_sem.at[layer], coarse_recv_sem.at[layer], me, other
        )

        def relay(ref):
            return remote(ref, ref, relay_send.at[layer], relay_recv.at[layer], me, other)

        def near_term(low, high):
            return dot(halo[layer], hot_far[: 2 * rows, low:high])

        def away_term(low, high):
            return dot(coarse[layer], hot_far[2 * rows :, low:high], ((0,), (0,)))

        def edge_phase(last_term):
            total = None
            for low, high in wide:
                hidden = silu(before[:, low:high] + last_term(low, high)).astype(bf16)
                mlp = dot(wo_turned[...], hidden) + column(1, layer)
                updated = edges[:, low:high].astype(f32) + layer_norm(mlp, column(2, layer), column(3, layer))
                fresh = jnp.where(live[:, low:high], updated, 0.0).astype(bf16)
                edges[:, low:high] = fresh
                term = dot(fresh, incidence[:, low:high], ((1,), (1,)))
                total = term if total is None else total + term
            partial[...] = total
            agg_send[layer] = total.astype(bf16)

        @pl.when(core == lead)
        def _():
            for side in (1, 0) if layer else (0, 1):
                if layer == 0 and side == 0:
                    pl.when(me != 1)(halo_arrival(0, 0).wait_recv)
                else:
                    halo_arrival(layer, side).wait_recv()
                relay(halo_part(layer, side)).start()
            before[...] = before[...] + near_term(0, mine)
            relay(every).wait_recv()
            edge_phase(away_term)

        @pl.when(core != lead)
        def _():
            all_coarse.wait_recv()
            relay(every).start()
            before[...] = before[...] + away_term(0, mine)
            relay(halo.at[layer]).wait_recv()
            edge_phase(near_term)

        swap = remote(
            agg_send.at[layer], agg_recv.at[layer], agg_sems.at[layer, 0], agg_sems.at[layer, 1], me, other
        )
        swap.start()
        if layer == layers - 1:
            keep = pltpu.make_async_copy(edges.at[here], edges_out.at[:, my_slots], out_sems.at[0])
            keep.start()
            give = remote(
                edges.at[there], edges_out.at[:, my_slots], out_sems.at[1], out_sems.at[2], me, other
            )
            give.start()
        swap.wait_recv()
        aggregate = (partial[...] + agg_recv[layer].astype(f32)).astype(bf16)
        node_hidden = silu(node_first + dot(weights[layer, :, at_aggregate], aggregate)).astype(bf16)
        node_mlp = dot(vo_turned[...], node_hidden) + column(5, layer)
        nodes[...] = (
            nodes[...].astype(f32) + layer_norm(node_mlp, column(6, layer), column(7, layer))
        ).astype(bf16)
        swap.wait_send()

    nodes_out[...] = nodes[here, :]
    for ref, index in ((nodes.at[here], 0), (edges.at[here], 1), (vectors.at[:, :, here], 2), (weights.at[:, here], 3)):
        remote(ref, ref, w_send.at[index], w_recv.at[index], me, other).wait_send()

    def sent(ref, sem):
        remote(ref, ref, sem, w_recv.at[0], me, other).wait_send()

    @pl.when(core == lead)
    def _():
        for layer in range(layers):
            sent(halo.at[layer], relay_send.at[layer])
        for layer in range(1, layers):
            sent(halo.at[layer], halo_send.at[layer])
        one = part_send.at[0]
        pl.when(me == 0)(lambda: sent(one, halo_send.at[0]))
        pl.when(me == 1)(lambda: sent(weights.at[0, :, pl.ds(0, 3 * rows)], halo_send.at[0]))
        pl.when(me > 1)(lambda: sent(halo.at[0], halo_send.at[0]))

    @pl.when(core != lead)
    def _():
        for layer in range(layers):
            sent(coarse_part(layer), relay_send.at[layer])
            sent(coarse_part(layer), coarse_send_sem.at[layer])

    keep.wait()
    give.wait_send()
    got = edges_out.at[:, other_slots]
    remote(got, got, out_sems.at[1], out_sems.at[2], me, other).wait_recv()


def put(nodes, edges, nodes_out, edges_out, sems):
    copies = [
        pltpu.make_async_copy(edges, edges_out, sems.at[0]),
        pltpu.make_async_copy(nodes, nodes_out, sems.at[1]),
    ]
    for copy in copies:
        copy.start()
    for copy in copies:
        copy.wait()


def on_device(
    patches,
    node_latents,
    edge_latents,
    senders,
    receivers,
    edge_count,
    edge_in_weight,
    edge_in_bias,
    edge_out_weight,
    edge_out_bias,
    edge_gain,
    edge_shift,
    node_in_weight,
    node_in_bias,
    node_out_weight,
    node_out_bias,
    node_gain,
    node_shift,
):
    half, rows = node_latents.shape
    slots = edge_latents.shape[1]
    layers = edge_in_weight.shape[0]
    width = 2 * half
    mine = slots // 2
    top = rows // 8
    far_rows = -(-(patches - 3) * top // 128) * 128
    vmem = pltpu.VMEM
    dma = pltpu.SemaphoreType.DMA
    groups = 5 + layers
    anywhere = pl.BlockSpec(memory_space=pl.ANY)
    results = pl.pallas_call(
        functools.partial(kernel, patches),
        out_shape=(
            vmem((half, rows), bf16),
            vmem((half, slots), bf16),
        ),
        in_specs=[anywhere] * 17,
        out_specs=(pl.BlockSpec(memory_space=vmem),) * 2,
        scratch_shapes=[
            vmem((width, rows), bf16),
            vmem((width, mine), bf16),
            vmem((layers, width, 7 * width), bf16),
            vmem((8, layers, width), f32),
            vmem((width, 8 * layers), f32),
            vmem((layers, width, 2 * rows), bf16),
            vmem((layers, far_rows, width), bf16),
            vmem((layers, width, rows), bf16),
            vmem((layers, top, width), bf16),
            vmem((layers, width, rows), bf16),
            vmem((layers, width, rows), bf16),
            vmem((width, rows), f32),
            vmem((width, 2 * rows), bf16),
            vmem((2 * rows, mine), bf16),
            vmem((2 * rows + far_rows, mine), bf16),
            vmem((rows, mine), bf16),
            vmem((width, mine), f32),
            vmem((2, slots), jnp.int32),
            pltpu.SMEM((1,), jnp.int32),
            vmem((width, width), bf16),
            vmem((width, width), bf16),
            dma((2,)),
            dma((groups,)),
            dma((4,)),
            dma((groups,)),
            dma((layers,)),
            dma((layers, 2)),
            dma((layers,)),
            dma((layers,)),
            dma((layers,)),
            dma((layers,)),
            dma((layers, 2)),
            dma((3,)),
            pltpu.SemaphoreType.REGULAR,
            pltpu.SemaphoreType.REGULAR,
        ],
        compiler_params=pltpu.CompilerParams(collective_id=0, has_side_effects=True, vmem_limit_bytes=56 * 2**20),
    )(
        node_latents,
        edge_latents,
        senders.reshape(1, slots),
        receivers.reshape(1, slots),
        edge_count,
        edge_in_weight,
        edge_out_weight,
        node_in_weight,
        node_out_weight,
        edge_in_bias,
        edge_out_bias,
        edge_gain,
        edge_shift,
        node_in_bias,
        node_out_bias,
        node_gain,
        node_shift,
    )
    return pl.pallas_call(
        put,
        out_shape=(
            jax.ShapeDtypeStruct((half, rows), bf16),
            jax.ShapeDtypeStruct((half, slots), bf16),
        ),
        in_specs=[pl.BlockSpec(memory_space=vmem)] * 2,
        out_specs=(anywhere, anywhere),
        scratch_shapes=[dma((2,))],
        compiler_params=pltpu.CompilerParams(vmem_limit_bytes=4 * 2**20),
    )(*results)


def solution(mesh):
    by_width = P(None, "width")
    return jax.shard_map(
        functools.partial(on_device, mesh.shape["patch"]),
        mesh=mesh,
        in_specs=(
            P("width", "patch"),
            P("width", "patch"),
            P("patch"),
            P("patch"),
            P("patch"),
            P(None, "width", None),
            by_width,
            P(None, "width", None),
            by_width,
            by_width,
            by_width,
            P(None, "width", None),
            by_width,
            P(None, "width", None),
            by_width,
            by_width,
            by_width,
        ),
        out_specs=(P("width", "patch"), P("width", "patch")),
        check_vma=False,
    )
```

```python
import functools

import jax
import jax.numpy as jnp
from jax import lax
from jax.experimental import pallas as pl
from jax.experimental.pallas import tpu as pltpu
from jax.sharding import PartitionSpec as P

MESH = pl.DeviceIdType.MESH
epsilon = 1e-05
bf16 = jnp.bfloat16
f32 = jnp.float32


def dot(left, right, dims=((1,), (0,))):
    return lax.dot_general(left, right, (dims, ((), ())), preferred_element_type=f32)


def silu(v):
    h = 0.5 * v
    return h + h * jnp.tanh(h)


def layer_norm(values, gain, shift):
    width = values.shape[0]
    mean = jnp.sum(values, axis=0, keepdims=True) / width
    square = jnp.sum(values * values, axis=0, keepdims=True) / width
    return (values - mean) * lax.rsqrt(square - mean * mean + epsilon) * gain + shift


def kernel(
    patches,
    nodes_in,
    edges_in,
    senders_in,
    receivers_in,
    count_in,
    wi_in,
    wo_in,
    vi_in,
    vo_in,
    *rest,
):
    vector_in = rest[:8]
    nodes_out, edges_out = rest[8:10]
    (
        nodes,
        edges,
        weights,
        vectors,
        columns,
        halo,
        coarse,
        part_send,
        coarse_send,
        agg_send,
        agg_recv,
        partial,
        own,
        hot_own,
        hot_far,
        incidence,
        before,
        graph_ref,
        count_ref,
        wo_turned,
        vo_turned,
        graph_sem,
        local_sem,
        w_send,
        w_recv,
        halo_send,
        halo_recv,
        relay_send,
        relay_recv,
        agg_sems,
        out_sems,
        mate,
        all_in,
    ) = rest[10:]
    layers = weights.shape[0]
    half = nodes_in.shape[0]
    width = 2 * half
    rows = nodes_in.shape[1]
    slots = edges_in.shape[1]
    mine = slots // 2
    top = coarse_send.shape[1]
    far = patches - 3
    lead = 1

    me = lax.axis_index("patch")
    odd = lax.rem(me, 2)
    core = lax.axis_index("width")
    other = 1 - core
    here = pl.ds(pl.multiple_of(core * half, half), half)
    there = pl.ds(pl.multiple_of(other * half, half), half)
    my_slots = pl.ds(pl.multiple_of(core * mine, mine), mine)
    other_slots = pl.ds(pl.multiple_of(other * mine, mine), mine)

    def remote(src, dst, send, recv, patch, width_index):
        return pltpu.make_async_remote_copy(
            src_ref=src,
            dst_ref=dst,
            send_sem=send,
            recv_sem=recv,
            device_id={"patch": patch, "width": width_index},
            device_id_type=MESH,
        )

    at_sender, at_edge, at_receiver, at_wo, at_node, at_aggregate, at_vo = (
        slice(k * width, (k + 1) * width) for k in range(7)
    )

    def weight(source, layer, first_column, target, count=1):
        from_ = source.at[layer, :, pl.ds(first_column, count * width)]
        to = weights.at[layer, here, pl.ds(target.start, count * width)]
        return from_, to

    def layer_rest(layer):
        return [
            weight(wo_in, layer, 0, at_wo),
            weight(vi_in, layer, 0, at_node, 2),
            weight(vo_in, layer, 0, at_vo),
        ]

    def layer_ends(layer):
        return [
            weight(wi_in, layer, 0, at_edge),
            weight(wi_in, layer, 2 * width, at_receiver),
        ]

    groups = [
        ("nodes", [(nodes_in, nodes.at[here])], nodes.at[there]),
        ("sender", [weight(wi_in, 0, width, at_sender)], weights.at[0, there, at_sender]),
        ("ends", layer_ends(0), weights.at[0, there, pl.ds(width, 2 * width)]),
        ("edges", None, edges.at[there]),
        (
            "vectors",
            [(source, vectors.at[index, :, here]) for index, source in enumerate(vector_in)],
            vectors.at[:, :, there],
        ),
        ("rest", layer_rest(0), weights.at[0, there, pl.ds(3 * width, 4 * width)]),
    ]
    for layer in range(1, layers):
        groups.append(
            (
                layer,
                [weight(wi_in, layer, width, at_sender)] + layer_ends(layer) + layer_rest(layer),
                weights.at[layer, there],
            )
        )
    place = {group[0]: index for index, group in enumerate(groups)}
    send_of = {"nodes": 0, "edges": 1, "vectors": 2}
    mine_of = {
        "nodes": nodes.at[here],
        "sender": weights.at[0, here, at_sender],
        "ends": weights.at[0, here, pl.ds(width, 2 * width)],
        "edges": edges.at[here],
        "vectors": vectors.at[:, :, here],
        "rest": weights.at[0, here, pl.ds(3 * width, 4 * width)],
    } | {layer: weights.at[layer, here] for layer in range(1, layers)}

    barrier = pltpu.get_barrier_semaphore()

    @pl.when(core == lead)
    def _():
        pl.semaphore_signal(barrier, inc=1, device_id={"patch": me, "width": other}, device_id_type=MESH)

    def greet(step, carry):
        target = lax.rem(me + step, patches)

        @pl.when((target != 0) | (me == 1))
        def _():
            pl.semaphore_signal(
                pltpu.get_barrier_semaphore(),
                inc=1,
                device_id={"patch": target, "width": lead},
                device_id_type=MESH,
            )

        return carry

    lax.fori_loop(1, patches, greet, 0)

    count_copy = pltpu.make_async_copy(count_in, count_ref, graph_sem.at[1])
    graph_copies = [
        pltpu.make_async_copy(source, graph_ref.at[pl.ds(k, 1)], graph_sem.at[0])
        for k, source in enumerate((senders_in, receivers_in))
    ]

    def locals_of(index):
        name, copies, _ = groups[index]
        if name == "edges":
            copies = [(edges_in.at[:, my_slots], edges.at[here])]
        return [pltpu.make_async_copy(source, target, local_sem.at[index]) for source, target in copies]

    for index in range(2):
        for copy in locals_of(index):
            copy.start()
    for copy in [count_copy] + graph_copies:
        copy.start()
    for index in range(2, len(groups)):
        for copy in locals_of(index):
            copy.start()

    @pl.when(core != lead)
    def _():
        pl.semaphore_wait(barrier, 1)
        pl.semaphore_signal(mate, inc=1, device_id={"patch": me, "width": lead}, device_id_type=MESH)

    @pl.when(core == lead)
    def _():
        pl.semaphore_wait(mate, 1)

    for index, (name, copies, _) in enumerate(groups):
        if name == "edges":
            copies = [(edges_in.at[:, other_slots], edges.at[here])]
        for source, target in copies:
            remote(source, target, w_send.at[send_of.get(name, 3)], w_recv.at[index], me, other).start()

    def local_arrive(name):
        ref = mine_of[name]
        pltpu.make_async_copy(ref, ref, local_sem.at[place[name]]).wait()

    def arrive(name):
        if name not in ("nodes", "sender"):
            local_arrive(name)
        ref = groups[place[name]][2]
        remote(ref, ref, w_send.at[send_of.get(name, 3)], w_recv.at[place[name]], me, other).wait_recv()

    def hot(index, iota, scale=0.5):
        return jnp.where(iota == index, scale, 0.0).astype(bf16)

    def masks():
        count_copy.wait()
        pltpu.make_async_copy(graph_ref, graph_ref, graph_sem.at[0]).wait()
        sender = graph_ref[0:1, my_slots]
        receiver = graph_ref[1:2, my_slots] - me * rows
        slot = lax.broadcasted_iota(jnp.int32, (1, mine), 1) + core * mine
        live = slot < count_ref[0]
        owner = sender // rows
        within = sender - owner * rows
        distance = lax.rem(me - owner + patches, patches)
        node_iota = lax.broadcasted_iota(jnp.int32, (rows, mine), 0)
        hot_own[:rows] = hot(jnp.where(distance == 0, within, -1), node_iota)
        hot_own[rows:] = hot(receiver, node_iota)
        hot_far[:rows] = hot(jnp.where(distance == 1, within, -1), node_iota)
        hot_far[rows : 2 * rows] = hot(jnp.where(distance == patches - 1, within, -1), node_iota)
        far_index = jnp.where((distance >= 2) & (distance <= patches - 2), (distance - 2) * top + within, -1)
        hot_far[2 * rows :] = hot(far_index, lax.broadcasted_iota(jnp.int32, (coarse.shape[1], mine), 0))
        incidence[...] = hot(jnp.where(live, receiver, -1), node_iota, 1.0)
        return live

    pad = coarse.shape[1] - far * top
    if pad:
        for layer in range(layers):
            coarse[layer, far * top :, :] = jnp.zeros((pad, width), bf16)

    def halo_part(layer, side):
        return halo.at[layer, :, pl.ds(pl.multiple_of(side * rows, rows), rows)]

    def halo_copy(layer, side):
        return remote(
            part_send.at[layer],
            halo_part(layer, side),
            halo_send.at[layer],
            halo_recv.at[layer, side],
            lax.rem(me + 1 + side * (patches - 2), patches),
            lead,
        )

    def halo_arrival(layer, side):
        ref = halo_part(layer, side)
        return remote(ref, ref, halo_send.at[layer], halo_recv.at[layer, side], me, other)

    def coarse_part(layer):
        return coarse.at[layer, pl.ds(0, far * top)]

    def spread_coarse(layer):
        def send(target, step):
            remote(
                coarse_send.at[layer],
                coarse.at[layer, pl.ds(pl.multiple_of((step - 2) * top, top), top)],
                halo_send.at[layer],
                halo_recv.at[layer, 0],
                target,
                1 - lead,
            ).start()

        def spread(turn, carry):
            step = patches - 2 - turn
            pl.when(me + step < patches)(lambda: send(me + step, step))
            pl.when(me - step >= 0)(lambda: send(me - step, patches - step))
            return carry

        lax.fori_loop(0, far, spread, 0)

    def send_halo(layer):
        if layer == 0:
            pl.semaphore_wait(barrier, jnp.where(me == 0, 2, 2 * (patches - 1)))

            @pl.when(me != 0)
            def _():
                pl.semaphore_signal(
                    all_in, inc=1, device_id={"patch": me, "width": other}, device_id_type=MESH
                )

            @pl.when(me == 1)
            def _():
                pl.semaphore_signal(all_in, inc=1, device_id={"patch": 0, "width": other}, device_id_type=MESH)
                halo_arrival(0, 0).wait_recv()
                remote(
                    halo_part(0, 0), halo_part(0, 1), halo_send.at[0], halo_recv.at[0, 1], patches - 1, lead
                ).start()

            pl.when(me != 0)(halo_copy(0, 1 - odd).start)
        else:
            halo_copy(layer, 1 - odd).start()
        halo_copy(layer, odd).start()

    def send_coarse(layer):
        if layer == 0:
            pl.semaphore_wait(all_in, 1)
        spread_coarse(layer)

    def column(index, layer):
        position = index * layers + layer
        return columns[:, position : position + 1]

    wide = [(k * mine // 2, (k + 1) * mine // 2) for k in range(2)]
    for layer in range(layers):
        if layer == 0:
            local_arrive("nodes")
            local_arrive("sender")
            arrive("nodes")
            arrive("sender")
        else:
            arrive(layer)
        part = dot(weights[layer, :, at_sender], nodes[...])
        part_send[layer] = part.astype(bf16)
        pl.when(core == lead)(functools.partial(send_halo, layer))

        @pl.when(core != lead)
        def _():
            coarse_send[layer] = part.T[:top].astype(bf16)
            send_coarse(layer)

        if layer == 0:
            live = masks()
            arrive("ends")
        own[:, :rows] = part.astype(bf16)
        own[:, rows:] = dot(weights[layer, :, at_receiver], nodes[...]).astype(bf16)
        if layer == 0:
            arrive("edges")
            arrive("vectors")
            flat = vectors[...].reshape(8 * layers, width)
            columns[...] = flat.T
        before[...] = (
            0.5 * (dot(weights[layer, :, at_edge], edges[...]) + column(0, layer)) + dot(own[...], hot_own[...])
        )
        if layer == 0:
            arrive("rest")
        node_first = dot(weights[layer, :, at_node], nodes[...]) + column(4, layer)
        wo_turned[...] = weights[layer, :, at_wo].T
        vo_turned[...] = weights[layer, :, at_vo].T

        every = coarse_part(layer)
        all_coarse = remote(
            every, every, halo_send.at[layer], halo_recv.at[layer, 0], me, other
        )

        def relay(ref):
            return remote(ref, ref, relay_send.at[layer], relay_recv.at[0], me, other)

        def near_term(low, high):
            return dot(halo[layer], hot_far[: 2 * rows, low:high])

        def away_term(low, high):
            return dot(coarse[layer], hot_far[2 * rows :, low:high], ((0,), (0,)))

        def edge_phase(last_term):
            total = None
            for low, high in wide:
                h = before[:, low:high] + last_term(low, high)
                hidden = (h + h * jnp.tanh(h)).astype(bf16)
                mlp = dot(wo_turned[...], hidden) + column(1, layer)
                updated = edges[:, low:high].astype(f32) + layer_norm(mlp, column(2, layer), column(3, layer))
                fresh = jnp.where(live[:, low:high], updated, 0.0).astype(bf16)
                edges[:, low:high] = fresh
                term = dot(fresh, incidence[:, low:high], ((1,), (1,)))
                total = term if total is None else total + term
            partial[...] = total
            agg_send[layer] = total.astype(bf16)

        @pl.when(core == lead)
        def _():
            for side in (1, 0) if layer else (0, 1):
                if layer == 0 and side == 0:
                    pl.when(me != 1)(halo_arrival(0, 0).wait_recv)
                else:
                    halo_arrival(layer, side).wait_recv()
                relay(halo_part(layer, side)).start()
            before[...] = before[...] + near_term(0, mine)
            relay(every).wait_recv()
            edge_phase(away_term)

        @pl.when(core != lead)
        def _():
            all_coarse.wait_recv()
            relay(every).start()
            before[...] = before[...] + away_term(0, mine)
            relay(halo.at[layer]).wait_recv()
            edge_phase(near_term)

        swap = remote(
            agg_send.at[layer], agg_recv.at[layer], agg_sems.at[0], agg_sems.at[1], me, other
        )
        swap.start()
        if layer == layers - 1:
            keep = pltpu.make_async_copy(edges.at[here], edges_out.at[:, my_slots], out_sems.at[0])
            keep.start()
            give = remote(
                edges.at[there], edges_out.at[:, my_slots], out_sems.at[1], out_sems.at[2], me, other
            )
            give.start()
        swap.wait_recv()
        aggregate = (partial[...] + agg_recv[layer].astype(f32)).astype(bf16)
        node_hidden = silu(node_first + dot(weights[layer, :, at_aggregate], aggregate)).astype(bf16)
        node_mlp = dot(vo_turned[...], node_hidden) + column(5, layer)
        nodes[...] = (
            nodes[...].astype(f32) + layer_norm(node_mlp, column(6, layer), column(7, layer))
        ).astype(bf16)
        swap.wait_send()

    nodes_out[...] = nodes[here, :]
    for ref, index in ((nodes.at[here], 0), (edges.at[here], 1), (vectors.at[:, :, here], 2), (weights.at[:, here], 3)):
        remote(ref, ref, w_send.at[index], w_recv.at[index], me, other).wait_send()

    def sent(ref, sem):
        remote(ref, ref, sem, w_recv.at[0], me, other).wait_send()

    @pl.when(core == lead)
    def _():
        for layer in range(layers):
            sent(halo.at[layer], relay_send.at[layer])
        for layer in range(1, layers):
            sent(halo.at[layer], halo_send.at[layer])
        one = part_send.at[0]
        pl.when(me == 0)(lambda: sent(one, halo_send.at[0]))
        pl.when(me == 1)(lambda: sent(weights.at[0, :, pl.ds(0, 3 * rows)], halo_send.at[0]))
        pl.when(me > 1)(lambda: sent(halo.at[0], halo_send.at[0]))

    @pl.when(core != lead)
    def _():
        for layer in range(layers):
            sent(coarse_part(layer), relay_send.at[layer])
            sent(coarse_part(layer), halo_send.at[layer])

    keep.wait()
    give.wait_send()
    got = edges_out.at[:, other_slots]
    remote(got, got, out_sems.at[1], out_sems.at[2], me, other).wait_recv()


def put(nodes, edges, nodes_out, edges_out, sems):
    copies = [
        pltpu.make_async_copy(edges, edges_out, sems.at[0]),
        pltpu.make_async_copy(nodes, nodes_out, sems.at[1]),
    ]
    for copy in copies:
        copy.start()
    for copy in copies:
        copy.wait()


def on_device(
    patches,
    node_latents,
    edge_latents,
    senders,
    receivers,
    edge_count,
    edge_in_weight,
    edge_in_bias,
    edge_out_weight,
    edge_out_bias,
    edge_gain,
    edge_shift,
    node_in_weight,
    node_in_bias,
    node_out_weight,
    node_out_bias,
    node_gain,
    node_shift,
):
    half, rows = node_latents.shape
    slots = edge_latents.shape[1]
    layers = edge_in_weight.shape[0]
    width = 2 * half
    mine = slots // 2
    top = rows // 8
    far_rows = -(-(patches - 3) * top // 128) * 128
    vmem = pltpu.VMEM
    dma = pltpu.SemaphoreType.DMA
    groups = 5 + layers
    anywhere = pl.BlockSpec(memory_space=pl.ANY)
    results = pl.pallas_call(
        functools.partial(kernel, patches),
        out_shape=(
            vmem((half, rows), bf16),
            vmem((half, slots), bf16),
        ),
        in_specs=[anywhere] * 17,
        out_specs=(pl.BlockSpec(memory_space=vmem),) * 2,
        scratch_shapes=[
            vmem((width, rows), bf16),
            vmem((width, mine), bf16),
            vmem((layers, width, 7 * width), bf16),
            vmem((8, layers, width), f32),
            vmem((width, 8 * layers), f32),
            vmem((layers, width, 2 * rows), bf16),
            vmem((layers, far_rows, width), bf16),
            vmem((layers, width, rows), bf16),
            vmem((layers, top, width), bf16),
            vmem((layers, width, rows), bf16),
            vmem((layers, width, rows), bf16),
            vmem((width, rows), f32),
            vmem((width, 2 * rows), bf16),
            vmem((2 * rows, mine), bf16),
            vmem((2 * rows + far_rows, mine), bf16),
            vmem((rows, mine), bf16),
            vmem((width, mine), f32),
            vmem((2, slots), jnp.int32),
            pltpu.SMEM((1,), jnp.int32),
            vmem((width, width), bf16),
            vmem((width, width), bf16),
            dma((2,)),
            dma((groups,)),
            dma((4,)),
            dma((groups,)),
            dma((layers,)),
            dma((layers, 2)),
            dma((layers,)),
            dma((1,)),
            dma((2,)),
            dma((3,)),
            pltpu.SemaphoreType.REGULAR,
            pltpu.SemaphoreType.REGULAR,
        ],
        compiler_params=pltpu.CompilerParams(collective_id=0, has_side_effects=True, vmem_limit_bytes=56 * 2**20),
    )(
        node_latents,
        edge_latents,
        senders.reshape(1, slots),
        receivers.reshape(1, slots),
        edge_count,
        edge_in_weight,
        edge_out_weight,
        node_in_weight,
        node_out_weight,
        edge_in_bias,
        edge_out_bias,
        edge_gain,
        edge_shift,
        node_in_bias,
        node_out_bias,
        node_gain,
        node_shift,
    )
    return pl.pallas_call(
        put,
        out_shape=(
            jax.ShapeDtypeStruct((half, rows), bf16),
            jax.ShapeDtypeStruct((half, slots), bf16),
        ),
        in_specs=[pl.BlockSpec(memory_space=vmem)] * 2,
        out_specs=(anywhere, anywhere),
        scratch_shapes=[dma((2,))],
        compiler_params=pltpu.CompilerParams(vmem_limit_bytes=4 * 2**20),
    )(*results)


def solution(mesh):
    by_width = P(None, "width")
    return jax.shard_map(
        functools.partial(on_device, mesh.shape["patch"]),
        mesh=mesh,
        in_specs=(
            P("width", "patch"),
            P("width", "patch"),
            P("patch"),
            P("patch"),
            P("patch"),
            P(None, "width", None),
            by_width,
            P(None, "width", None),
            by_width,
            by_width,
            by_width,
            P(None, "width", None),
            by_width,
            P(None, "width", None),
            by_width,
            by_width,
            by_width,
        ),
        out_specs=(P("width", "patch"), P("width", "patch")),
        check_vma=False,
    )
```
